32 devices in a mesh: seq: 8 (over y, x, core), head: 4 (over z).
Axes of the slice: x: 2, y: 2, z: 4, core: 2. Of those that a mesh axis runs over, the one named last changes fastest.
Arguments:
- queries: bfloat16 [2048, 4096], P('seq', 'head'), may hold values from -7.1875 to 7.1875
- keys: bfloat16 [2048, 1024], P(('seq', 'head')), may hold values from -7.1875 to 7.1875
- values: bfloat16 [2048, 1024], P(('seq', 'head')), may hold values from -6 to 6
- outputs: bfloat16 [2048, 4096], P('seq', 'head'), may hold values from -1.1953125 to 1.1953125
- out_grad: bfloat16 [2048, 4096], P('seq', 'head'), may hold values from -6 to 6
- log_norm: float32 [32, 2048], P('head', 'seq'), as said below
- block_order: int32 [16], replicated, may hold values from 0 to 15, as said below
Outputs:
- query_grad: bfloat16 [2048, 4096], P('seq', 'head')
- key_gradient_rows: bfloat16 [2048, 1024], P(('seq', 'head'))
- value_gradient_rows: bfloat16 [2048, 1024], P(('seq', 'head'))
The draws below stay inside these ranges and needn't reach their ends.
Inputs may be any that keep to these rules, and one draw needn't show every extreme that they name: `block_order`: A permutation of 0 to 15. log_norm[h, i] lies within 0.6 of one plus the natural logarithm of 1 + pos[i].
All inputs are finite; a program needn't handle non-finite values.
Results may differ from the reference program's by a relative error of at most 0.014.
Values may be sent and summed in bfloat16 or wider, within the bound.
A program may use at most 192 MiB of HBM per device.

```python
import jax
import jax.numpy as jnp
from jax import lax

QUERY_HEADS = 32
KEY_VALUE_HEADS = 8
HEAD_SIZE = 128
TOK_DEV = 256
SEQUENCE_TOKENS = 2048
N_SEQ = 8


def order_helper(key):
    return jax.random.permutation(jax.random.fold_in(key, 7), 2 * N_SEQ).astype(jnp.int32)


def draw_block_order(key, part):
    return order_helper(key)


def draw_log_norm(key, part):
    order = order_helper(key)
    half = TOK_DEV // 2
    rows = jnp.arange(SEQUENCE_TOKENS, dtype=jnp.int32)
    pos = (order[rows // half] * half + rows % half).astype(jnp.float32)
    base = jnp.log(1.0 + pos)[None, :] + 1.0
    noise = jax.random.uniform(jax.random.fold_in(key, 11), (QUERY_HEADS, SEQUENCE_TOKENS), jnp.float32, -0.3, 0.3)
    return (base + noise).astype(jnp.float32)


def block_levels(rng, shape, shards, smallest, top_value):
    level = 1.0
    for position, parts in shards:
        heights = jax.random.uniform(jax.random.fold_in(jax.random.fold_in(rng, 6), position), (parts,), jnp.float32, smallest / len(shards), top_value / len(shards))
        level = level * jnp.repeat(jnp.exp(heights), shape[position] // parts).reshape((-1,) + (1,) * (len(shape) - 1 - position))
    return level


def gaussian(key, extent, width, most, pieces=(), kind=jnp.bfloat16):
    entries = jax.random.normal(key, extent, jnp.float32) * width
    if len(pieces) > 0:
        entries = block_levels(key, extent, pieces, -0.22, 0.18) * entries
    return jnp.clip(entries, min=-most, max=most).astype(kind)


def setup_inputs(seed: int = 0) -> dict:
    streams_of = jax.random.split(jax.random.key(seed), 8)
    queries = gaussian(streams_of[0], (SEQUENCE_TOKENS, QUERY_HEADS * HEAD_SIZE), 1.2, 7.1875, ((0, 8), (1, 4)))
    keys = gaussian(streams_of[1], (SEQUENCE_TOKENS, KEY_VALUE_HEADS * HEAD_SIZE), 1.2, 7.1875, ((0, 32),))
    values = gaussian(streams_of[2], (SEQUENCE_TOKENS, KEY_VALUE_HEADS * HEAD_SIZE), 1.0, 6.0, ((0, 32),))
    outputs = gaussian(streams_of[3], (SEQUENCE_TOKENS, QUERY_HEADS * HEAD_SIZE), 0.2, 1.1953125, ((0, 8), (1, 4)))
    out_grad = gaussian(streams_of[4], (SEQUENCE_TOKENS, QUERY_HEADS * HEAD_SIZE), 1.0, 6.0, ((0, 8), (1, 4)))
    log_norm = draw_log_norm(jax.random.fold_in(streams_of[7], 71), 0)
    block_order = draw_block_order(jax.random.fold_in(streams_of[7], 71), 0)
    return {"queries": queries, "keys": keys, "values": values, "outputs": outputs, "out_grad": out_grad, "log_norm": log_norm, "block_order": block_order}


def token_positions(block_order):
    half = TOK_DEV // 2
    rows = jnp.arange(SEQUENCE_TOKENS, dtype=jnp.int32)
    return (block_order[rows // half] * half + rows % half).astype(jnp.int32)


def reference(queries, keys, values, outputs, out_grad, log_norm, block_order):
    scale = HEAD_SIZE ** -0.5
    group_ratio = QUERY_HEADS // KEY_VALUE_HEADS
    pos = token_positions(block_order)
    delta = jnp.sum((out_grad.astype(jnp.float32) * outputs.astype(jnp.float32)).reshape(SEQUENCE_TOKENS, QUERY_HEADS, HEAD_SIZE), -1)
    qblock = 512 if SEQUENCE_TOKENS % 512 == 0 else SEQUENCE_TOKENS
    nblocks = SEQUENCE_TOKENS // qblock

    def queries_per_group(g):
        kg = lax.dynamic_slice_in_dim(keys, g * HEAD_SIZE, HEAD_SIZE, 1).astype(jnp.float32)
        vg = lax.dynamic_slice_in_dim(values, g * HEAD_SIZE, HEAD_SIZE, 1).astype(jnp.float32)
        qg = lax.dynamic_slice_in_dim(queries, g * group_ratio * HEAD_SIZE, group_ratio * HEAD_SIZE, 1).reshape(SEQUENCE_TOKENS, group_ratio, HEAD_SIZE)
        dg = lax.dynamic_slice_in_dim(out_grad, g * group_ratio * HEAD_SIZE, group_ratio * HEAD_SIZE, 1).reshape(SEQUENCE_TOKENS, group_ratio, HEAD_SIZE)
        lg = lax.dynamic_slice_in_dim(log_norm, g * group_ratio, group_ratio, 0)
        eg = lax.dynamic_slice_in_dim(delta, g * group_ratio, group_ratio, 1)

        def step(carry, b):
            keys_gradient, values_gradient = carry
            start = (b * qblock).astype(jnp.int32)
            qb = lax.dynamic_slice_in_dim(qg, start, qblock, 0).astype(jnp.float32)
            db = lax.dynamic_slice_in_dim(dg, start, qblock, 0).astype(jnp.float32)
            lb = lax.dynamic_slice_in_dim(lg, start, qblock, 1)
            eb = lax.dynamic_slice_in_dim(eg, start, qblock, 0)
            qpos = lax.dynamic_slice_in_dim(pos, start, qblock, 0)
            scores = jnp.einsum("trd,nd->rtn", qb, kg) * scale
            visible = pos[None, :] <= qpos[:, None]
            prob = jnp.where(visible[None], jnp.exp(scores - lb[:, :, None]), 0.0)
            dprob = jnp.einsum("trd,nd->rtn", db, vg)
            dscore = prob * (dprob - eb.T[:, :, None])
            prob_low = prob.astype(jnp.bfloat16).astype(jnp.float32)
            dscore_low = dscore.astype(jnp.bfloat16).astype(jnp.float32)
            values_gradient = values_gradient + jnp.einsum("rtn,trd->nd", prob_low, db)
            keys_gradient = keys_gradient + scale * jnp.einsum("rtn,trd->nd", dscore_low, qb)
            queries_gradient = scale * jnp.einsum("rtn,nd->trd", dscore_low, kg)
            return (keys_gradient, values_gradient), queries_gradient.astype(jnp.bfloat16)

        zeros = jnp.zeros((SEQUENCE_TOKENS, HEAD_SIZE), jnp.float32)
        (keys_gradient, values_gradient), queries_gradient = lax.scan(step, (zeros, zeros), jnp.arange(nblocks, dtype=jnp.int32))
        return queries_gradient.reshape(SEQUENCE_TOKENS, group_ratio * HEAD_SIZE), keys_gradient.astype(jnp.bfloat16), values_gradient.astype(jnp.bfloat16)

    queries_gradient, keys_gradient, values_gradient = lax.map(queries_per_group, jnp.arange(KEY_VALUE_HEADS, dtype=jnp.int32))
    query_grad = jnp.transpose(queries_gradient, (1, 0, 2)).reshape(SEQUENCE_TOKENS, QUERY_HEADS * HEAD_SIZE)
    key_gradient_rows = jnp.transpose(keys_gradient, (1, 0, 2)).reshape(SEQUENCE_TOKENS, KEY_VALUE_HEADS * HEAD_SIZE)
    value_gradient_rows = jnp.transpose(values_gradient, (1, 0, 2)).reshape(SEQUENCE_TOKENS, KEY_VALUE_HEADS * HEAD_SIZE)
    return (query_grad, key_gradient_rows, value_gradient_rows)
```

```python
import functools
import math

import jax
import jax.numpy as jnp
from jax import lax
from jax.experimental import pallas as pl
from jax.experimental.pallas import tpu as pltpu
from jax.sharding import PartitionSpec as P

QUERY_HEADS = 32
KEY_VALUE_HEADS = 8
HEAD_SIZE = 128
MESH = pl.DeviceIdType.MESH
NT = (((1,), (1,)), ((), ()))
F32 = jnp.float32
BF16 = jnp.bfloat16


def kernel(
    n_seq,
    n_head,
    q_in,
    k_in,
    v_in,
    o_in,
    do_in,
    lse_in,
    order,
    dq_out,
    dk_out,
    dv_out,
    qs,
    dos,
    o_all,
    do_all,
    lse,
    delta,
    kv,
    acc,
    dqt,
    dq_send,
    dq_recv,
    part_send,
    part_recv,
    last_send,
    last_recv,
    load_sem,
    first_send_sem,
    first_recv_sem,
    pair_send_sem,
    pair_recv_sem,
    kv_send_sem,
    kv_recv_sem,
    part_send_sem,
    part_recv_sem,
    last_send_sem,
    last_recv_sem,
    dq_sem,
):
    D = HEAD_SIZE
    R = QUERY_HEADS // KEY_VALUE_HEADS
    chips = n_seq // 2
    bits = (chips - 1).bit_length()
    steps = 2 * chips
    rows = q_in.shape[0]
    half = rows // 2
    piece = k_in.shape[0]
    me_s = lax.axis_index("seq")
    head = lax.axis_index("head")
    core = me_s % 2
    chip = me_s // 2
    mate = (core + 1) % 2
    mate_id = (chip * 2 + mate, head)
    scale = D ** (-0.5)

    def flip(a, d):
        return sum(((a // 2**i) % 2 + (d // 2**i) % 2) % 2 * 2**i for i in range(bits))

    def peer(d):
        return (flip(chip, d) * 2 + core, head)

    near = [(a, b) for b in range(n_head) for a in range(2) if (a, b) != (0, 0)]

    def near_at(a, b):
        return (core + a) % 2, (head + b) % n_head

    def lanes(start, size):
        return pl.ds(pl.multiple_of(start, D), size)

    loads = [
        pltpu.make_async_copy(o_in, o_all, load_sem.at[0]),
        pltpu.make_async_copy(do_in, do_all, load_sem.at[1]),
        pltpu.make_async_copy(lse_in, lse.at[0], load_sem.at[2]),
    ]
    mine = lanes((2 * head + core) * D, D)
    own_rows = pl.ds(pl.multiple_of(head * piece, piece), piece)
    loads.append(pltpu.make_async_copy(k_in.at[:, mine], kv.at[0, 0, 0, own_rows, :], load_sem.at[3]))
    loads.append(pltpu.make_async_copy(v_in.at[:, mine], kv.at[0, 0, 1, own_rows, :], load_sem.at[4]))
    for r in range(R):
        cols = lanes((core * R + r) * D, D)
        loads.append(pltpu.make_async_copy(q_in.at[:, cols], qs.at[0, r], load_sem.at[5 + r]))
        loads.append(pltpu.make_async_copy(do_in.at[:, cols], dos.at[0, r], load_sem.at[5 + R + r]))
    for copy in loads:
        copy.start()

    barrier = pltpu.get_barrier_semaphore()
    for a, b in near:
        c2, h2 = near_at(a, b)
        pl.semaphore_signal(barrier, inc=1, device_id=(chip * 2 + c2, h2), device_id_type=MESH)
    for d in range(1, chips):
        pl.semaphore_signal(barrier, inc=1, device_id=peer(d), device_id_type=MESH)
    pl.semaphore_wait(barrier, len(near) + chips - 1)

    first = {}
    for a, b in near:
        c2, h2 = near_at(a, b)
        for j, src in enumerate((k_in, v_in)):
            first[a, b, j] = pltpu.make_async_remote_copy(
                src_ref=src.at[:, lanes((2 * h2 + c2) * D, D)],
                dst_ref=kv.at[0, a, j, own_rows, :],
                send_sem=first_send_sem.at[a * n_head + b, j],
                recv_sem=first_recv_sem.at[a * n_head + b, j],
                device_id=(chip * 2 + c2, h2),
                device_id_type=MESH,
            )
    for key in sorted(first):
        first[key].start()
    pair = []

    def to_mate(src, dst, i):
        return pltpu.make_async_remote_copy(
            src_ref=src,
            dst_ref=dst,
            send_sem=pair_send_sem.at[i],
            recv_sem=pair_recv_sem.at[i],
            device_id=mate_id,
            device_id_type=MESH,
        )

    for r in range(R):
        cols = lanes((mate * R + r) * D, D)
        pair.append(to_mate(q_in.at[:, cols], qs.at[1, r], r))
        pair.append(to_mate(do_in.at[:, cols], dos.at[1, r], R + r))
    pair.append(to_mate(lse_in, lse.at[1], 2 * R))
    for copy in pair:
        copy.start()

    for copy in loads:
        copy.wait()
    for i in range(2 * R):
        prod = o_all[:, i * D : (i + 1) * D].astype(F32) * do_all[:, i * D : (i + 1) * D].astype(F32)
        delta[0, pl.ds(i, 1), :] = jnp.sum(prod.T, axis=0, keepdims=True)
    dqt[...] = jnp.zeros_like(dqt)
    acc[...] = jnp.zeros_like(acc)

    def kv_copy(d, hf):
        return pltpu.make_async_remote_copy(
            src_ref=kv.at[0, hf],
            dst_ref=kv.at[d, hf],
            send_sem=kv_send_sem.at[d, hf],
            recv_sem=kv_recv_sem.at[d, hf],
            device_id=peer(d),
            device_id_type=MESH,
        )

    for hf in range(2):
        for a, b, j in sorted(first):
            if a == hf:
                first[a, b, j].wait_recv()
        for d in range(1, min(chips, 3)):
            kv_copy(d, hf).start()
    for d in range(3, chips):
        for hf in range(2):
            kv_copy(d, hf).start()

    send_delta = to_mate(delta.at[0], delta.at[1], 2 * R + 1)
    send_delta.start()
    pair.append(send_delta)
    for copy in pair:
        copy.wait_recv()

    def part_copy(d, hf):
        return pltpu.make_async_remote_copy(
            src_ref=part_send.at[d, hf],
            dst_ref=part_recv.at[d, hf],
            send_sem=part_send_sem.at[d, hf],
            recv_sem=part_recv_sem.at[d, hf],
            device_id=peer(d),
            device_id_type=MESH,
        )

    dq_copy = pltpu.make_async_remote_copy(
        src_ref=dq_send.at[1],
        dst_ref=dq_recv,
        send_sem=dq_sem.at[0],
        recv_sem=dq_sem.at[1],
        device_id=mate_id,
        device_id_type=MESH,
    )

    def spots(index, shape, dim):
        off = lax.broadcasted_iota(jnp.int32, shape, dim)
        b0 = order[2 * index]
        b1 = order[2 * index + 1]
        return off + jnp.where(off < half, b0 * half, b1 * half - half)

    def step(t, carry):
        d = ((t + 1) // 2) % chips
        hf = (t + 1) % 2

        @pl.when(d > 0)
        def _():
            kv_copy(d, hf).wait_recv()

        def inner(i, carry):
            rr = (i + t // (steps - 1)) % 2
            kk = kv[d, hf, 0]
            vv = kv[d, hf, 1]
            kt = kk.T
            k_at = spots(flip(chip, d) * 2 + (core + hf) % 2, (rows, 1), 0)
            q_at = spots(chip * 2 + (core + rr) % 2, (1, rows), 1)
            mask = k_at <= q_at
            dk = None
            dv = None
            for r in range(R):
                qr = qs[rr, r]
                dor = dos[rr, r]
                s = lax.dot_general(kk, qr, NT, preferred_element_type=F32)
                dp = lax.dot_general(vv, dor, NT, preferred_element_type=F32)
                row = pl.ds(core * R + r, 1)
                l2 = lse[rr, row, :] * math.log2(math.e)
                dl = delta[rr, row, :]
                prob = jnp.where(mask, jnp.exp2(s * (scale * math.log2(math.e)) - l2), 0.0)
                ds = (prob * (dp - dl)).astype(BF16)
                tv = jnp.dot(prob.astype(BF16), dor, preferred_element_type=F32)
                tk = jnp.dot(ds, qr, preferred_element_type=F32)
                dv = tv if dv is None else dv + tv
                dk = tk if dk is None else dk + tk
                dqt[rr, r] += jnp.dot(kt, ds, preferred_element_type=F32)
            acc[t, 0] += dk
            acc[t, 1] += dv

            @pl.when(t == steps - 1)
            def _():
                for r in range(R):
                    dq_send[rr, :, r * D : (r + 1) * D] = (dqt[rr, r] * scale).T.astype(BF16)

            @pl.when(jnp.logical_and(t == steps - 1, i == 0))
            def _():
                dq_copy.start()

            return carry

        lax.fori_loop(0, 2, inner, 0)

        @pl.when(d > 0)
        def _():
            part_send[d, hf] = acc[t].astype(BF16)
            part_copy(d, hf).start()

        return carry

    lax.fori_loop(0, steps, step, 0)

    def last_copy(a, b):
        c2, h2 = near_at(a, b)
        return pltpu.make_async_remote_copy(
            src_ref=last_send.at[a, :, pl.ds(pl.multiple_of(h2 * piece, piece), piece), :],
            dst_ref=last_recv.at[2 * head + core],
            send_sem=last_send_sem.at[a * n_head + b],
            recv_sem=last_recv_sem.at[a * n_head + b],
            device_id=(chip * 2 + c2, h2),
            device_id_type=MESH,
        )

    for hf in range(2):
        own = steps - 1 if hf == 0 else 0

        def add(d, total):
            part_copy(d, hf).wait_recv()
            return total + part_recv[d, hf].astype(F32)

        total = acc[own]
        for d in range(1, chips):
            total = add(d, total)
        last_send[hf, 0] = (total[0] * scale).astype(BF16)
        last_send[hf, 1] = total[1].astype(BF16)
        for a, b in near:
            if a == hf:
                last_copy(a, b).start()
    last_recv[2 * head + core] = last_send[0, :, own_rows, :]
    dq_out[:, lanes(core * R * D, R * D)] = dq_send[0]
    dq_copy.wait_recv()
    dq_out[:, lanes(mate * R * D, R * D)] = dq_recv[...]
    for a, b in near:
        last_copy(a, b).wait_recv()
    for g in range(2 * n_head):
        dk_out[:, g * D : (g + 1) * D] = last_recv[g, 0]
        dv_out[:, g * D : (g + 1) * D] = last_recv[g, 1]

    for key in sorted(first):
        first[key].wait_send()
    for copy in pair:
        copy.wait_send()
    for d in range(1, chips):
        for hf in range(2):
            kv_copy(d, hf).wait_send()
            part_copy(d, hf).wait_send()
    dq_copy.wait_send()
    for a, b in near:
        last_copy(a, b).wait_send()


def local(n_seq, n_head, queries, keys, values, outputs, out_grad, log_norm, block_order):
    D = HEAD_SIZE
    R = QUERY_HEADS // KEY_VALUE_HEADS
    chips = n_seq // 2
    rows, width = queries.shape
    piece = keys.shape[0]
    heads = log_norm.shape[0]
    anywhere = pl.BlockSpec(memory_space=pl.ANY)
    vmem = pl.BlockSpec(memory_space=pltpu.VMEM)
    dma = pltpu.SemaphoreType.DMA
    return pl.pallas_call(
        functools.partial(kernel, n_seq, n_head),
        out_shape=(
            jax.ShapeDtypeStruct(queries.shape, BF16),
            jax.ShapeDtypeStruct(keys.shape, BF16),
            jax.ShapeDtypeStruct(values.shape, BF16),
        ),
        in_specs=[anywhere] * 6 + [pl.BlockSpec(memory_space=pltpu.SMEM)],
        out_specs=(vmem, vmem, vmem),
        scratch_shapes=[
            pltpu.VMEM((2, R, rows, D), BF16),
            pltpu.VMEM((2, R, rows, D), BF16),
            pltpu.VMEM((rows, width), BF16),
            pltpu.VMEM((rows, width), BF16),
            pltpu.VMEM((2, heads, rows), F32),
            pltpu.VMEM((2, heads, rows), F32),
            pltpu.VMEM((chips, 2, 2, rows, D), BF16),
            pltpu.VMEM((2 * chips, 2, rows, D), F32),
            pltpu.VMEM((2, R, D, rows), F32),
            pltpu.VMEM((2, rows, R * D), BF16),
            pltpu.VMEM((rows, R * D), BF16),
            pltpu.VMEM((chips, 2, 2, rows, D), BF16),
            pltpu.VMEM((chips, 2, 2, rows, D), BF16),
            pltpu.VMEM((2, 2, rows, D), BF16),
            pltpu.VMEM((2 * n_head, 2, piece, D), BF16),
            dma((5 + 2 * R,)),
            dma((2 * n_head, 2)),
            dma((2 * n_head, 2)),
            dma((2 * R + 2,)),
            dma((2 * R + 2,)),
            dma((chips, 2)),
            dma((chips, 2)),
            dma((chips, 2)),
            dma((chips, 2)),
            dma((2 * n_head,)),
            dma((2 * n_head,)),
            dma((2,)),
        ],
        compiler_params=pltpu.CompilerParams(
            collective_id=0, has_side_effects=True, vmem_limit_bytes=56 * 1024 * 1024
        ),
    )(queries, keys, values, outputs, out_grad, log_norm, block_order)


def solution(mesh):
    in_specs = (
        P("seq", "head"),
        P(("seq", "head"), None),
        P(("seq", "head"), None),
        P("seq", "head"),
        P("seq", "head"),
        P("head", "seq"),
        P(),
    )
    out_specs = (P("seq", "head"), P(("seq", "head"), None), P(("seq", "head"), None))
    body = functools.partial(local, mesh.shape["seq"], mesh.shape["head"])
    return jax.shard_map(body, mesh=mesh, in_specs=in_specs, out_specs=out_specs, check_vma=False)
```

```python
import functools
import math

import jax
import jax.numpy as jnp
from jax import lax
from jax.experimental import pallas as pl
from jax.experimental.pallas import tpu as pltpu
from jax.sharding import PartitionSpec as P

QUERY_HEADS = 32
KEY_VALUE_HEADS = 8
HEAD_SIZE = 128
MESH = pl.DeviceIdType.MESH
NT = (((1,), (1,)), ((), ()))
F32 = jnp.float32
BF16 = jnp.bfloat16
AHEAD = 3
LAG = 2


def kernel(
    n_seq,
    n_head,
    q_in,
    k_in,
    v_in,
    o_in,
    do_in,
    lse_in,
    order,
    dq_out,
    dk_out,
    dv_out,
    qs,
    dos,
    o_all,
    do_all,
    lse,
    delta,
    kv,
    acc,
    own_acc,
    dqt,
    dq_send,
    dq_recv,
    part_send,
    part_recv,
    last_send,
    last_recv,
    load_sem,
    first_send_sem,
    first_recv_sem,
    pair_send_sem,
    pair_recv_sem,
    kv_send_sem,
    kv_recv_sem,
    part_send_sem,
    part_recv_sem,
    last_send_sem,
    last_recv_sem,
    dq_sem,
):
    D = HEAD_SIZE
    R = QUERY_HEADS // KEY_VALUE_HEADS
    chips = n_seq // 2
    bits = (chips - 1).bit_length()
    steps = 2 * chips
    rows = q_in.shape[0]
    half = rows // 2
    piece = k_in.shape[0]
    me_s = lax.axis_index("seq")
    head = lax.axis_index("head")
    core = me_s % 2
    chip = me_s // 2
    mate = (core + 1) % 2
    mate_id = (chip * 2 + mate, head)
    scale = D ** (-0.5)

    def flip(a, d):
        return sum(((a // 2**i) % 2 + (d // 2**i) % 2) % 2 * 2**i for i in range(bits))

    def peer(d):
        return (flip(chip, d) * 2 + core, head)

    last = 2 * n_head - 1
    seg = min(chips, 4)
    chunks = chips // seg
    keys_here = seg * piece

    def block(t):
        m = (t + last) % (last + 1)
        end = t // last
        mid = ((t + last - 1) // last) * (1 - end)
        near_b = m // 4 + 1
        b = near_b + ((m // 2) % 2) * (n_head - 2 * near_b)
        return mid * (m % 2) + end, mid * b

    near = []
    for b in range(1, n_head // 2 + 1):
        for bb in sorted({b, n_head - b}):
            near += [(0, bb), (1, bb)]
    near.append((1, 0))

    def to_at(a, b):
        return (chip * 2 + (core + a) % 2, (head + b) % n_head)

    def from_at(a, b):
        return (chip * 2 + (core + a) % 2, (head + n_head - b) % n_head)

    def lanes(start, size):
        return pl.ds(pl.multiple_of(start, D), size)

    mine = lanes((2 * head + core) * D, D)
    kv_loads = [
        pltpu.make_async_copy(k_in.at[:, mine], kv.at[0, 0, 0, 0], load_sem.at[3]),
        pltpu.make_async_copy(v_in.at[:, mine], kv.at[0, 0, 1, 0], load_sem.at[4]),
    ]
    loads = [
        pltpu.make_async_copy(o_in, o_all, load_sem.at[0]),
        pltpu.make_async_copy(do_in, do_all, load_sem.at[1]),
        pltpu.make_async_copy(lse_in, lse.at[0], load_sem.at[2]),
    ]
    for r in range(R):
        cols = lanes((core * R + r) * D, D)
        loads.append(pltpu.make_async_copy(q_in.at[:, cols], qs.at[0, r], load_sem.at[5 + r]))
        loads.append(pltpu.make_async_copy(do_in.at[:, cols], dos.at[0, r], load_sem.at[5 + R + r]))
    for copy in kv_loads + loads:
        copy.start()

    barrier = pltpu.get_barrier_semaphore()
    for a, b in near:
        pl.semaphore_signal(barrier, inc=1, device_id=to_at(a, b), device_id_type=MESH)
    for d in range(1, chips):
        pl.semaphore_signal(barrier, inc=1, device_id=peer(d), device_id_type=MESH)
    pl.semaphore_wait(barrier, len(near) + chips - 1)

    def near_copy(a, b, j):
        target = to_at(a, b)
        src = (k_in, v_in)[j]
        return pltpu.make_async_remote_copy(
            src_ref=src.at[:, lanes((2 * target[1] + target[0] % 2) * D, D)],
            dst_ref=kv.at[a, b, j, 0],
            send_sem=first_send_sem.at[a * n_head + b, j],
            recv_sem=first_recv_sem.at[a * n_head + b, j],
            device_id=target,
            device_id_type=MESH,
        )

    def kv_copy(a, b, d):
        return pltpu.make_async_remote_copy(
            src_ref=kv.at[a, b, :, 0],
            dst_ref=kv.at[a, b, :, d],
            send_sem=kv_send_sem.at[a * n_head + b, d],
            recv_sem=kv_recv_sem.at[a * n_head + b, d],
            device_id=peer(d),
            device_id_type=MESH,
        )

    def part_copy(a, b, d):
        return pltpu.make_async_remote_copy(
            src_ref=part_send.at[a, b, d],
            dst_ref=part_recv.at[a, b, d],
            send_sem=part_send_sem.at[a * n_head + b, d],
            recv_sem=part_recv_sem.at[a * n_head + b, d],
            device_id=peer(d),
            device_id_type=MESH,
        )

    def last_copy(a, b):
        return pltpu.make_async_remote_copy(
            src_ref=last_send.at[a, b],
            dst_ref=last_recv.at[2 * head + core],
            send_sem=last_send_sem.at[a * n_head + b],
            recv_sem=last_recv_sem.at[a * n_head + b],
            device_id=from_at(a, b),
            device_id_type=MESH,
        )

    def to_mate(src, dst, i):
        return pltpu.make_async_remote_copy(
            src_ref=src,
            dst_ref=dst,
            send_sem=pair_send_sem.at[i],
            recv_sem=pair_recv_sem.at[i],
            device_id=mate_id,
            device_id_type=MESH,
        )

    def forward(t):
        a, b = block(t)
        near_copy(a, b, 0).wait_recv()
        near_copy(a, b, 1).wait_recv()
        for d in range(1, chips):
            kv_copy(a, b, d).start()

    for copy in kv_loads:
        copy.wait()
    for d in range(1, chips):
        kv_copy(0, 0, d).start()
    for a, b in near:
        near_copy(a, b, 0).start()
        near_copy(a, b, 1).start()
    pair = []
    for r in range(R):
        cols = lanes((mate * R + r) * D, D)
        pair.append(to_mate(q_in.at[:, cols], qs.at[1, r], r))
        pair.append(to_mate(do_in.at[:, cols], dos.at[1, r], R + r))
    pair.append(to_mate(lse_in, lse.at[1], 2 * R))
    for copy in pair:
        copy.start()

    for copy in loads:
        copy.wait()
    for i in range(2 * R):
        prod = o_all[:, i * D : (i + 1) * D].astype(F32) * do_all[:, i * D : (i + 1) * D].astype(F32)
        delta[0, pl.ds(i, 1), :] = jnp.sum(prod.T, axis=0, keepdims=True)
    dqt[...] = jnp.zeros_like(dqt)
    send_delta = to_mate(delta.at[0], delta.at[1], 2 * R + 1)
    forward(1)
    send_delta.start()
    pair.append(send_delta)
    for t in range(2, AHEAD):
        forward(t)
    for copy in pair:
        copy.wait_recv()

    dq_copy = pltpu.make_async_remote_copy(
        src_ref=dq_send.at[1],
        dst_ref=dq_recv,
        send_sem=dq_sem.at[0],
        recv_sem=dq_sem.at[1],
        device_id=mate_id,
        device_id_type=MESH,
    )

    def reduce(t):
        a, b = block(t)
        total = own_acc[a, b]
        for d in range(1, chips):
            part_copy(a, b, d).wait_recv()
            total = total + part_recv[a, b, d].astype(F32)
        last_send[a, b, 0] = (total[0] * scale).astype(BF16)
        last_send[a, b, 1] = total[1].astype(BF16)

    def spots(index):
        off = lax.broadcasted_iota(jnp.int32, (1, rows), 1)
        b0 = order[2 * index]
        b1 = order[2 * index + 1]
        return off + jnp.where(off < half, b0 * half, b1 * half - half)

    def step(t, carry):
        a, b = block(t)
        from_core = (core + a) % 2
        from_row = ((head + n_head - b) % n_head) * piece

        @pl.when(t + AHEAD <= last)
        def _():
            forward(t + AHEAD)

        def chunk(c, carry):
            d0 = c * seg
            for e in range(seg):
                if e > 0:
                    kv_copy(a, b, d0 + e).wait_recv()
                elif chunks > 1:

                    @pl.when(c > 0)
                    def _():
                        kv_copy(a, b, d0).wait_recv()

            def inner(i, carry):
                rr = (i + t // last) % 2
                kk = kv[a, b, 0, pl.ds(d0, seg)].reshape(keys_here, D)
                vv = kv[a, b, 1, pl.ds(d0, seg)].reshape(keys_here, D)
                kt = kk.T
                off = lax.broadcasted_iota(jnp.int32, (keys_here, 1), 0)
                k_at = off
                for e in range(seg):
                    index = flip(chip, d0 + e) * 2 + from_core
                    base = order[2 * index + from_row // half] * half + from_row % half - e * piece
                    k_at = jnp.where(off >= e * piece, off + base, k_at)
                q_at = spots(chip * 2 + (core + rr) % 2)
                mask = k_at <= q_at
                dk = None
                dv = None
                for r in range(R):
                    qr = qs[rr, r]
                    dor = dos[rr, r]
                    s = lax.dot_general(kk, qr, NT, preferred_element_type=F32)
                    dp = lax.dot_general(vv, dor, NT, preferred_element_type=F32)
                    row = pl.ds(core * R + r, 1)
                    l2 = lse[rr, row, :] * math.log2(math.e)
                    dl = delta[rr, row, :]
                    prob = jnp.where(mask, jnp.exp2(s * (scale * math.log2(math.e)) - l2), 0.0)
                    ds = (prob * (dp - dl)).astype(BF16)
                    tv = jnp.dot(prob.astype(BF16), dor, preferred_element_type=F32)
                    tk = jnp.dot(ds, qr, preferred_element_type=F32)
                    dv = tv if dv is None else dv + tv
                    dk = tk if dk is None else dk + tk
                    dqt[rr, r] += jnp.dot(kt, ds, preferred_element_type=F32)

                @pl.when(i == 0)
                def _():
                    acc[0] = dk
                    acc[1] = dv

                @pl.when(i == 1)
                def _():
                    acc[0] += dk
                    acc[1] += dv

                @pl.when(jnp.logical_and(t == last, c == chunks - 1))
                def _():
                    for r in range(R):
                        dq_send[rr, :, r * D : (r + 1) * D] = (dqt[rr, r] * scale).T.astype(BF16)

                @pl.when(jnp.logical_and(jnp.logical_and(t == last, c == chunks - 1), i == 0))
                def _():
                    dq_copy.start()

                return carry

            lax.fori_loop(0, 2, inner, 0)
            for e in range(seg):
                here = slice(e * piece, (e + 1) * piece)
                if e > 0:
                    part_send[a, b, d0 + e] = acc[:, here, :].astype(BF16)
                    part_copy(a, b, d0 + e).start()
                elif chunks > 1:

                    @pl.when(c == 0)
                    def _():
                        own_acc[a, b] = acc[:, here, :]

                    @pl.when(c > 0)
                    def _():
                        part_send[a, b, d0] = acc[:, here, :].astype(BF16)
                        part_copy(a, b, d0).start()

                else:
                    own_acc[a, b] = acc[:, here, :]
            return carry

        if chunks > 1:
            lax.fori_loop(0, chunks, chunk, 0)
        else:
            chunk(0, 0)

        @pl.when(t == LAG)
        def _():
            reduce(0)

        @pl.when(t > LAG)
        def _():
            reduce(t - LAG)
            last_copy(*block(t - LAG)).start()

        return carry

    lax.fori_loop(0, last + 1, step, 0)
    for t in range(last + 1 - LAG, last + 1):
        reduce(t)
        last_copy(*block(t)).start()
    last_recv[2 * head + core] = last_send[0, 0]
    dq_out[:, lanes(core * R * D, R * D)] = dq_send[0]
    dq_copy.wait_recv()
    dq_out[:, lanes(mate * R * D, R * D)] = dq_recv[...]
    for a, b in near:
        last_copy(a, b).wait_recv()
    for g in range(2 * n_head):
        dk_out[:, g * D : (g + 1) * D] = last_recv[g, 0]
        dv_out[:, g * D : (g + 1) * D] = last_recv[g, 1]

    for copy in pair:
        copy.wait_send()
    dq_copy.wait_send()
    for a, b in near:
        near_copy(a, b, 0).wait_send()
        near_copy(a, b, 1).wait_send()
        last_copy(a, b).wait_send()
    for a, b in [(0, 0)] + near:
        for d in range(1, chips):
            kv_copy(a, b, d).wait_send()
            part_copy(a, b, d).wait_send()


def local(n_seq, n_head, queries, keys, values, outputs, out_grad, log_norm, block_order):
    D = HEAD_SIZE
    R = QUERY_HEADS // KEY_VALUE_HEADS
    chips = n_seq // 2
    rows, width = queries.shape
    piece = keys.shape[0]
    heads = log_norm.shape[0]
    anywhere = pl.BlockSpec(memory_space=pl.ANY)
    vmem = pl.BlockSpec(memory_space=pltpu.VMEM)
    dma = pltpu.SemaphoreType.DMA
    return pl.pallas_call(
        functools.partial(kernel, n_seq, n_head),
        out_shape=(
            jax.ShapeDtypeStruct(queries.shape, BF16),
            jax.ShapeDtypeStruct(keys.shape, BF16),
            jax.ShapeDtypeStruct(values.shape, BF16),
        ),
        in_specs=[anywhere] * 6 + [pl.BlockSpec(memory_space=pltpu.SMEM)],
        out_specs=(vmem, vmem, vmem),
        scratch_shapes=[
            pltpu.VMEM((2, R, rows, D), BF16),
            pltpu.VMEM((2, R, rows, D), BF16),
            pltpu.VMEM((rows, width), BF16),
            pltpu.VMEM((rows, width), BF16),
            pltpu.VMEM((2, heads, rows), F32),
            pltpu.VMEM((2, heads, rows), F32),
            pltpu.VMEM((2, n_head, 2, chips, piece, D), BF16),
            pltpu.VMEM((2, min(chips, 4) * piece, D), F32),
            pltpu.VMEM((2, n_head, 2, piece, D), F32),
            pltpu.VMEM((2, R, D, rows), F32),
            pltpu.VMEM((2, rows, R * D), BF16),
            pltpu.VMEM((rows, R * D), BF16),
            pltpu.VMEM((2, n_head, chips, 2, piece, D), BF16),
            pltpu.VMEM((2, n_head, chips, 2, piece, D), BF16),
            pltpu.VMEM((2, n_head, 2, piece, D), BF16),
            pltpu.VMEM((2 * n_head, 2, piece, D), BF16),
            dma((5 + 2 * R,)),
            dma((2 * n_head, 2)),
            dma((2 * n_head, 2)),
            dma((2 * R + 2,)),
            dma((2 * R + 2,)),
            dma((2 * n_head, chips)),
            dma((2 * n_head, chips)),
            dma((2 * n_head, chips)),
            dma((2 * n_head, chips)),
            dma((2 * n_head,)),
            dma((2 * n_head,)),
            dma((2,)),
        ],
        compiler_params=pltpu.CompilerParams(
            collective_id=0, has_side_effects=True, vmem_limit_bytes=56 * 1024 * 1024
        ),
    )(queries, keys, values, outputs, out_grad, log_norm, block_order)


def solution(mesh):
    in_specs = (
        P("seq", "head"),
        P(("seq", "head"), None),
        P(("seq", "head"), None),
        P("seq", "head"),
        P("seq", "head"),
        P("head", "seq"),
        P(),
    )
    out_specs = (P("seq", "head"), P(("seq", "head"), None), P(("seq", "head"), None))
    body = functools.partial(local, mesh.shape["seq"], mesh.shape["head"])
    return jax.shard_map(body, mesh=mesh, in_specs=in_specs, out_specs=out_specs, check_vma=False)
```
